32 devices in a mesh: rep: 1 (over z), shard: 32 (over y, x, core).
Axes of the slice: x: 4, y: 4, z: 1, core: 2. Of those that a mesh axis runs over, the one named last changes fastest.
The devices are a block of a 4x4x8 slice.
Arguments:
- ratings: float32 [8192, 8192], P(('rep', 'shard'))
- obs_mask: int32 [8192, 8192], P(('rep', 'shard'))
- step_counts: int32 [32, 32], P(('rep', 'shard'))
- user_init: float32 [8192, 128], P(('rep', 'shard'))
- item_init: float32 [8192, 128], P(('rep', 'shard'))
Outputs:
- output 1: float32 [8192, 128], P(('rep', 'shard'))
- output 2: float32 [8192, 128], P(('rep', 'shard'))
All inputs are finite; a program needn't handle non-finite values.
Results may differ from the reference program's by a relative error of at most 0.00136811.
Values are sent between devices in bfloat16 or wider.
A program may use at most 768 MiB of HBM per device.

```python
import math
import jax
import jax.numpy as jnp
from jax import lax

GROUP_SIZE = 32
FACTOR_RANK = 128
ASPECT = 1
ITEMS_DEV = 256
STEPS_MAX = 6
EPOCHS = 2

USERS_DEV = ASPECT * ITEMS_DEV
NUM_USERS = GROUP_SIZE * USERS_DEV
NUM_ITEMS = GROUP_SIZE * ITEMS_DEV
TRUE_RANK = FACTOR_RANK // 4
STEP_SIZE = 0.4 * math.sqrt(FACTOR_RANK) / (USERS_DEV + FACTOR_RANK)
DECAY_RATE = 0.1 * ITEMS_DEV / math.sqrt(FACTOR_RANK)


def draw_layout(layout_key):
    key_list = jax.random.split(layout_key, 5)
    density_pct = jax.random.randint(key_list[0], (GROUP_SIZE, 1, GROUP_SIZE, 1), 10, 41)
    coin_draws = jax.random.randint(key_list[1], (GROUP_SIZE, USERS_DEV, GROUP_SIZE, ITEMS_DEV), 0, 100)
    obs_mask = (coin_draws < density_pct).astype(jnp.int32).reshape(NUM_USERS, NUM_ITEMS)
    slot_count = GROUP_SIZE * GROUP_SIZE
    step_flat = jax.random.randint(key_list[2], (slot_count,), 1, STEPS_MAX + 1)
    top_pos = jax.random.randint(key_list[3], (), 0, slot_count)
    low_pos = (top_pos + 1 + jax.random.randint(key_list[4], (), 0, slot_count - 1)) % slot_count
    slot_ids = jnp.arange(slot_count)
    step_flat = jnp.where(slot_ids == top_pos, STEPS_MAX, jnp.where(slot_ids == low_pos, 1, step_flat))
    return obs_mask, step_flat.reshape(GROUP_SIZE, GROUP_SIZE).astype(jnp.int32)


def setup_inputs(seed: int = 0, part: int = 0) -> dict:
    base_key = jax.random.fold_in(jax.random.key(seed), part)
    key_list = jax.random.split(base_key, 6)
    user_true = jax.random.normal(key_list[0], (NUM_USERS, TRUE_RANK), jnp.float32)
    item_true = jax.random.normal(key_list[1], (NUM_ITEMS, TRUE_RANK), jnp.float32)
    noise_term = 0.3 * jax.random.normal(key_list[2], (NUM_USERS, NUM_ITEMS), jnp.float32)
    ratings = jnp.dot(user_true, item_true.T) / math.sqrt(TRUE_RANK) + noise_term
    obs_mask, step_counts = draw_layout(key_list[3])
    factor_scale = FACTOR_RANK ** -0.25
    user_init = factor_scale * jax.random.normal(key_list[4], (NUM_USERS, FACTOR_RANK), jnp.float32)
    item_init = factor_scale * jax.random.normal(key_list[5], (NUM_ITEMS, FACTOR_RANK), jnp.float32)
    return {"ratings": ratings, "obs_mask": obs_mask, "step_counts": step_counts, "user_init": user_init, "item_init": item_init}


def reference(ratings, obs_mask, step_counts, user_init, item_init):
    rating_blocks = ratings.reshape(GROUP_SIZE, USERS_DEV, GROUP_SIZE, ITEMS_DEV)
    mask_blocks = obs_mask.reshape(GROUP_SIZE, USERS_DEV, GROUP_SIZE, ITEMS_DEV)
    user_blocks = user_init.reshape(GROUP_SIZE, USERS_DEV, FACTOR_RANK)
    item_blocks = item_init.reshape(GROUP_SIZE, ITEMS_DEV, FACTOR_RANK)
    row_ids = jnp.arange(GROUP_SIZE)

    def block_update(block_args):
        row_id, col_id, user_blk, item_blk = block_args
        rating_blk = rating_blocks[row_id, :, col_id, :]
        seen_blk = mask_blocks[row_id, :, col_id, :] != 0

        def grad_step(step_idx, inner_in):
            user_now, item_now = inner_in
            user_half = user_now.astype(jnp.bfloat16)
            item_half = item_now.astype(jnp.bfloat16)
            approx = jnp.dot(user_half, item_half.T, preferred_element_type=jnp.float32)
            err_half = jnp.where(seen_blk, approx - rating_blk, 0.0).astype(jnp.bfloat16)
            grad_user = jnp.dot(err_half, item_half, preferred_element_type=jnp.float32) + DECAY_RATE * user_now
            grad_item = jnp.dot(err_half.T, user_half, preferred_element_type=jnp.float32) + DECAY_RATE * item_now
            return user_now - STEP_SIZE * grad_user, item_now - STEP_SIZE * grad_item

        return lax.fori_loop(0, step_counts[row_id, col_id], grad_step, (user_blk, item_blk))

    def sub_epoch(sweep_idx, carry_in):
        user_cur, held_items = carry_in
        col_ids = (row_ids + sweep_idx) % GROUP_SIZE
        user_new, item_new = lax.map(block_update, (row_ids, col_ids, user_cur, held_items))
        return user_new, jnp.roll(item_new, -1, axis=0)

    user_fin, item_fin = lax.fori_loop(0, EPOCHS * GROUP_SIZE, sub_epoch, (user_blocks, item_blocks))
    return user_fin.reshape(NUM_USERS, FACTOR_RANK), item_fin.reshape(NUM_ITEMS, FACTOR_RANK)
```

```python
import functools
import math

import jax
import jax.numpy as jnp
from jax import lax
from jax.experimental import pallas as pl
from jax.experimental.pallas import tpu as pltpu
from jax.sharding import PartitionSpec as P

EPOCHS = 2
STEPS_MAX = 6
MESH = pl.DeviceIdType.MESH


def factor_kernel(group, ratings, obs_mask, counts, user_init, item_init, user_out, item_out,
                  items, user_t, target, rating_in, mask_in,
                  send_sem, recv_sem, rating_sem, mask_sem):
    users_dev, rank = user_init.shape
    items_dev = item_init.shape[0]
    sweeps = EPOCHS * group
    eta = 0.4 * math.sqrt(rank) / (users_dev + rank)
    lam = 0.1 * items_dev / math.sqrt(rank)
    me = lax.axis_index("shard")
    left = lax.rem(me + group - 1, group)
    right = lax.rem(me + 1, group)

    def fetch(sweep):
        col = lax.rem(me + sweep, group)
        cols = pl.ds(pl.multiple_of(col * items_dev, items_dev), items_dev)
        half = lax.rem(sweep, 2)
        return (
            pltpu.make_async_copy(ratings.at[:, cols], rating_in.at[half], rating_sem.at[half]),
            pltpu.make_async_copy(obs_mask.at[:, cols], mask_in.at[half], mask_sem.at[half]),
        )

    def hop(sweep):
        return pltpu.make_async_remote_copy(
            src_ref=items.at[sweep],
            dst_ref=items.at[sweep + 1],
            send_sem=send_sem.at[sweep],
            recv_sem=recv_sem.at[sweep],
            device_id={"shard": left},
            device_id_type=MESH,
        )

    def prepare(sweep):
        for copy in fetch(sweep):
            copy.wait()
        half = lax.rem(sweep, 2)
        marked = jnp.where(mask_in[half] != 0, rating_in[half], jnp.inf)
        target[lax.rem(me + sweep, group)] = marked.T

    for copy in fetch(0) + fetch(1):
        copy.start()
    barrier = pltpu.get_barrier_semaphore()
    for neighbour in (left, right):
        pl.semaphore_signal(barrier, inc=1, device_id={"shard": neighbour}, device_id_type=MESH)
    pl.semaphore_wait(barrier, 2)

    user_t[...] = user_init[...].T
    items[0] = item_init[...]
    prepare(0)

    def sub_epoch(sweep, _):
        col = lax.rem(me + sweep, group)
        count = counts[0, col]

        @pl.when(sweep > 0)
        def _():
            hop(sweep - 1).wait_recv()

        for step in range(STEPS_MAX):
            active = step < count
            bound = jnp.where(active, jnp.inf, -jnp.inf)
            keep = jnp.where(active, 1.0 - eta * lam, 1.0)
            item_now = items[sweep]
            user_now = user_t[...]
            item_half = item_now.astype(jnp.bfloat16)
            user_half = user_now.astype(jnp.bfloat16)
            approx = jnp.dot(item_half, user_half, preferred_element_type=jnp.float32)
            goal = target[col]
            err = jnp.where(goal < bound, approx - goal, 0.0).astype(jnp.bfloat16)
            grad_item = lax.dot_general(err, user_half, (((1,), (1,)), ((), ())), preferred_element_type=jnp.float32)
            grad_user = lax.dot_general(item_half, err, (((0,), (0,)), ((), ())), preferred_element_type=jnp.float32)
            items[sweep] = keep * item_now - eta * grad_item
            user_t[...] = keep * user_now - eta * grad_user

        hop(sweep).start()

        @pl.when(sweep + 2 < group)
        def _():
            for copy in fetch(sweep + 2):
                copy.start()

        @pl.when(sweep + 1 < group)
        def _():
            prepare(sweep + 1)

        return 0

    lax.fori_loop(0, sweeps, sub_epoch, 0)
    user_out[...] = user_t[...].T
    hop(sweeps - 1).wait_recv()
    item_out[...] = items[sweeps]

    def drain(sweep, _):
        hop(sweep).wait_send()
        return 0

    lax.fori_loop(0, sweeps, drain, 0)


def solution(mesh):
    group = mesh.shape["shard"]
    row_spec = P(("rep", "shard"), None)

    def local_run(ratings, obs_mask, step_counts, user_init, item_init):
        users_dev, rank = user_init.shape
        items_dev = item_init.shape[0]
        sweeps = EPOCHS * group
        vmem = pl.BlockSpec(memory_space=pltpu.VMEM)
        hbm = pl.BlockSpec(memory_space=pl.ANY)
        return pl.pallas_call(
            functools.partial(factor_kernel, group),
            out_shape=(
                jax.ShapeDtypeStruct(user_init.shape, jnp.float32),
                jax.ShapeDtypeStruct(item_init.shape, jnp.float32),
            ),
            in_specs=[hbm, hbm, pl.BlockSpec(memory_space=pltpu.SMEM), vmem, vmem],
            out_specs=(vmem, vmem),
            scratch_shapes=[
                pltpu.VMEM((sweeps + 1, items_dev, rank), jnp.float32),
                pltpu.VMEM((rank, users_dev), jnp.float32),
                pltpu.VMEM((group, items_dev, users_dev), jnp.float32),
                pltpu.VMEM((2, users_dev, items_dev), jnp.float32),
                pltpu.VMEM((2, users_dev, items_dev), jnp.int32),
                pltpu.SemaphoreType.DMA((sweeps,)),
                pltpu.SemaphoreType.DMA((sweeps,)),
                pltpu.SemaphoreType.DMA((2,)),
                pltpu.SemaphoreType.DMA((2,)),
            ],
            compiler_params=pltpu.CompilerParams(
                collective_id=0, has_side_effects=True, vmem_limit_bytes=40 * 1024 * 1024
            ),
            name="factor_ring",
        )(ratings, obs_mask, step_counts, user_init, item_init)

    return jax.shard_map(local_run, mesh=mesh, in_specs=(row_spec,) * 5, out_specs=(row_spec, row_spec), check_vma=False)
```

```python
import functools
import math

import jax
import jax.numpy as jnp
from jax import lax
from jax.experimental import pallas as pl
from jax.experimental.pallas import tpu as pltpu
from jax.sharding import PartitionSpec as P

EPOCHS = 2
STEPS_MAX = 6
MESH = pl.DeviceIdType.MESH
F32 = jnp.float32
BF16 = jnp.bfloat16


def product(a, b, contract):
    return lax.dot_general(a, b, (contract, ((), ())), preferred_element_type=F32)


def factor_kernel(group, ratings, obs_mask, step_counts, user_init, item_init, user_out, item_out,
                  items, users, target, outbox, rating_in, mask_in, user_in, count_row, counts,
                  item_send, item_recv, user_send, user_recv, block_send, block_recv,
                  rating_sem, mask_sem, count_send, count_recv, init_sem):
    users_dev, rank = user_init.shape
    items_dev = item_init.shape[0]
    sweeps = EPOCHS * group
    laps = sweeps // 2
    eta = 0.4 * math.sqrt(rank) / (users_dev + rank)
    lam = 0.1 * items_dev / math.sqrt(rank)
    me = lax.axis_index("shard")
    side = lax.rem(me, 2)
    base = me - side
    mate = base + 1 - side
    left = lax.rem(me + group - 2, group)
    right = lax.rem(me + 2, group)

    def fetch(sweep):
        col = lax.rem(me + sweep, group)
        cols = pl.ds(pl.multiple_of(col * items_dev, items_dev), items_dev)
        half = lax.rem(sweep, 2)
        return (
            pltpu.make_async_copy(ratings.at[:, cols], rating_in.at[half], rating_sem.at[half]),
            pltpu.make_async_copy(obs_mask.at[:, cols], mask_in.at[half], mask_sem.at[half]),
        )

    def to_mate(src, dst, send_sem, recv_sem):
        return pltpu.make_async_remote_copy(
            src_ref=src, dst_ref=dst, send_sem=send_sem, recv_sem=recv_sem,
            device_id={"shard": mate}, device_id_type=MESH)

    def item_hop(lap):
        return pltpu.make_async_remote_copy(
            src_ref=items.at[lap], dst_ref=items.at[lap + 1], send_sem=item_send.at[0], recv_sem=item_recv.at[lap],
            device_id={"shard": left}, device_id_type=MESH)

    def user_hop(sweep):
        half = lax.rem(sweep, 2)
        return to_mate(users.at[sweep], users.at[sweep + 1], user_send.at[half], user_recv.at[half])

    def block_hop(sweep):
        col = lax.rem(me + sweep, group)
        half = lax.rem(sweep // 2, 2)
        return to_mate(outbox.at[half], target.at[side, col // 2], block_send.at[half], block_recv.at[sweep // 2])

    def count_hop():
        return to_mate(count_row.at[0], count_row.at[1], count_send, count_recv)

    def merged(sweep):
        for copy in fetch(sweep):
            copy.wait()
        half = lax.rem(sweep, 2)
        return jnp.where(mask_in[half] != 0, rating_in[half], jnp.inf).T

    def keep_block(sweep):
        target[side, lax.rem(me + sweep, group) // 2] = merged(sweep)

    def give_block(sweep):
        outbox[lax.rem(sweep // 2, 2)] = merged(sweep)
        block_hop(sweep).start()

    init_copies = (
        pltpu.make_async_copy(user_init, user_in, init_sem.at[0]),
        pltpu.make_async_copy(item_init, items.at[0], init_sem.at[1]),
        pltpu.make_async_copy(step_counts, count_row.at[0], init_sem.at[2]),
    )
    for copy in init_copies + fetch(0) + fetch(1):
        copy.start()
    barrier = pltpu.get_barrier_semaphore()
    for neighbour in (mate, left, right):
        pl.semaphore_signal(barrier, inc=1, device_id={"shard": neighbour}, device_id_type=MESH)
    for copy in init_copies:
        copy.wait()
    users[0] = user_in[...].T
    pltpu.async_copy(count_row.at[0], counts.at[0], init_sem.at[0]).wait()
    keep_block(0)
    pl.semaphore_wait(barrier, 3)
    count_hop().start()
    give_block(1)
    for copy in fetch(2) + fetch(3):
        copy.start()

    def run(sweep, lap, last_first):
        row = lax.rem(side + sweep, 2)
        col = lax.rem(base + row + sweep, group)
        count = counts[lax.rem(sweep, 2), 0, col]
        item = items.at[lap]
        user = users.at[sweep]
        goal_ref = target.at[row, col // 2]
        for step in range(STEPS_MAX):
            active = step < count
            bound = jnp.where(active, jnp.inf, -jnp.inf)
            keep = jnp.where(active, 1.0 - eta * lam, 1.0)
            item_now = item[...]
            user_now = user[...]
            item_half = item_now.astype(BF16)
            user_half = user_now.astype(BF16)
            approx = product(item_half, user_half, ((1,), (0,)))
            goal = goal_ref[...]
            err = jnp.where(goal < bound, approx - goal, 0.0).astype(BF16)
            item[...] = keep * item_now - eta * product(err, user_half, ((1,), (1,)))
            if last_first and step == STEPS_MAX - 1:
                last_first()
            user[...] = keep * user_now - eta * product(item_half, err, ((0,), (0,)))
        user_hop(sweep).start()

    def arrive_user(sweep):
        @pl.when(sweep > 0)
        def _():
            user_hop(sweep - 1).wait()

        @pl.when(sweep == 1)
        def _():
            count_hop().wait()
            pltpu.async_copy(count_row.at[1], counts.at[1], init_sem.at[0]).wait()

        @pl.when(jnp.logical_and(lax.rem(sweep, 2) == 1, sweep < group))
        def _():
            block_hop(sweep).wait_recv()

    def first_user(sweep, lap):
        arrive_user(sweep)

        @pl.when(lap > 0)
        def _():
            item_hop(lap - 1).wait_recv()

        run(sweep, lap, None)

    def second_user(sweep, lap):
        arrive_user(sweep)

        @pl.when(lap > 0)
        def _():
            item_hop(lap - 1).wait_send()

        run(sweep, lap, lambda: item_hop(lap).start())

    def lap_run(lap, _):
        second = 2 * lap + side

        @pl.when(jnp.logical_or(lap > 0, side == 1))
        def _():
            first_user(second - 1, lap)

        second_user(second, lap)

        @pl.when(2 * lap + 2 < group)
        def _():
            keep_block(2 * lap + 2)

            @pl.when(lap > 0)
            def _():
                block_hop(2 * lap - 1).wait_send()

            give_block(2 * lap + 3)

            @pl.when(2 * lap + 4 < group)
            def _():
                for copy in fetch(2 * lap + 4) + fetch(2 * lap + 5):
                    copy.start()

        return 0

    lax.fori_loop(0, laps, lap_run, 0)

    @pl.when(side == 0)
    def _():
        first_user(sweeps - 1, laps)

    @pl.when(side == 1)
    def _():
        item_hop(laps - 1).wait_recv()

    user_hop(sweeps - 1).wait()
    user_out[...] = users[sweeps].T
    item_out[...] = items[laps]
    item_hop(laps - 1).wait_send()
    block_hop(group - 3).wait_send()
    block_hop(group - 1).wait_send()


def solution(mesh):
    group = mesh.shape["shard"]
    row_spec = P(("rep", "shard"), None)

    def local_run(ratings, obs_mask, step_counts, user_init, item_init):
        users_dev, rank = user_init.shape
        items_dev = item_init.shape[0]
        sweeps = EPOCHS * group
        vmem = pl.BlockSpec(memory_space=pltpu.VMEM)
        hbm = pl.BlockSpec(memory_space=pltpu.HBM)
        dma = pltpu.SemaphoreType.DMA
        return pl.pallas_call(
            functools.partial(factor_kernel, group),
            out_shape=(
                jax.ShapeDtypeStruct(user_init.shape, F32),
                jax.ShapeDtypeStruct(item_init.shape, F32),
            ),
            in_specs=[hbm] * 5,
            out_specs=(vmem, vmem),
            scratch_shapes=[
                pltpu.VMEM((sweeps // 2 + 1, items_dev, rank), F32),
                pltpu.VMEM((sweeps + 1, rank, users_dev), F32),
                pltpu.VMEM((2, group // 2, items_dev, users_dev), F32),
                pltpu.VMEM((2, items_dev, users_dev), F32),
                pltpu.VMEM((2, users_dev, items_dev), F32),
                pltpu.VMEM((2, users_dev, items_dev), jnp.int32),
                pltpu.VMEM(user_init.shape, F32),
                pltpu.VMEM((2, *step_counts.shape), jnp.int32),
                pltpu.SMEM((2, *step_counts.shape), jnp.int32),
                dma((1,)),
                dma((sweeps // 2,)),
                dma((2,)),
                dma((2,)),
                dma((2,)),
                dma((group // 2,)),
                dma((2,)),
                dma((2,)),
                dma,
                dma,
                dma((3,)),
            ],
            compiler_params=pltpu.CompilerParams(
                collective_id=0, has_side_effects=True, vmem_limit_bytes=40 * 1024 * 1024
            ),
            name="factor_ring",
        )(ratings, obs_mask, step_counts, user_init, item_init)

    return jax.shard_map(local_run, mesh=mesh, in_specs=(row_spec,) * 5, out_specs=(row_spec, row_spec), check_vma=False)
```

```python
import functools
import math

import jax
import jax.numpy as jnp
from jax import lax
from jax.experimental import pallas as pl
from jax.experimental.pallas import tpu as pltpu
from jax.sharding import PartitionSpec as P

EPOCHS = 2
STEPS_MAX = 6
MESH = pl.DeviceIdType.MESH
F32 = jnp.float32
BF16 = jnp.bfloat16


def product(a, b, contract):
    return lax.dot_general(a, b, (contract, ((), ())), preferred_element_type=F32)


def factor_kernel(group, ratings, obs_mask, step_counts, user_init, item_init, user_out, item_out,
                  items, users, target, outbox, rating_in, mask_in, user_in, count_row, counts,
                  item_send, item_recv, user_send, user_recv, block_send, block_recv,
                  rating_sem, mask_sem, count_send, count_recv, init_sem):
    users_dev, rank = user_init.shape
    items_dev = item_init.shape[0]
    sweeps = EPOCHS * group
    laps = sweeps // 2
    eta = 0.4 * math.sqrt(rank) / (users_dev + rank)
    lam = 0.1 * items_dev / math.sqrt(rank)
    me = lax.axis_index("shard")
    side = lax.rem(me, 2)
    base = me - side
    mate = base + 1 - side
    left = lax.rem(me + group - 2, group)
    right = lax.rem(me + 2, group)

    def fetch(sweep):
        col = lax.rem(me + sweep, group)
        cols = pl.ds(pl.multiple_of(col * items_dev, items_dev), items_dev)
        half = lax.rem(sweep, 2)
        return (
            pltpu.make_async_copy(ratings.at[:, cols], rating_in.at[half], rating_sem.at[half]),
            pltpu.make_async_copy(obs_mask.at[:, cols], mask_in.at[half], mask_sem.at[half]),
        )

    def to_mate(src, dst, send_sem, recv_sem):
        return pltpu.make_async_remote_copy(
            src_ref=src, dst_ref=dst, send_sem=send_sem, recv_sem=recv_sem,
            device_id={"shard": mate}, device_id_type=MESH)

    def item_hop(lap):
        return pltpu.make_async_remote_copy(
            src_ref=items.at[lap], dst_ref=items.at[lap + 1], send_sem=item_send.at[0], recv_sem=item_recv.at[lap],
            device_id={"shard": left}, device_id_type=MESH)

    def user_hop(sweep):
        half = lax.rem(sweep, 2)
        return to_mate(users.at[sweep], users.at[sweep + 1], user_send.at[half], user_recv.at[half])

    def block_hop(sweep):
        col = lax.rem(me + sweep, group)
        half = lax.rem(sweep // 2, 2)
        return to_mate(outbox.at[half], target.at[side, col // 2], block_send.at[half], block_recv.at[sweep // 2])

    def count_hop():
        return to_mate(count_row.at[0], count_row.at[1], count_send, count_recv)

    def merged(sweep):
        for copy in fetch(sweep):
            copy.wait()
        half = lax.rem(sweep, 2)
        return jnp.where(mask_in[half] != 0, rating_in[half], jnp.inf).T

    def keep_block(sweep):
        target[side, lax.rem(me + sweep, group) // 2] = merged(sweep)

    def give_block(sweep):
        outbox[lax.rem(sweep // 2, 2)] = merged(sweep)
        block_hop(sweep).start()

    init_copies = (
        pltpu.make_async_copy(user_init, user_in, init_sem.at[0]),
        pltpu.make_async_copy(item_init, items.at[0], init_sem.at[1]),
        pltpu.make_async_copy(step_counts, count_row.at[0], init_sem.at[2]),
    )
    for copy in init_copies + fetch(0) + fetch(1):
        copy.start()
    barrier = pltpu.get_barrier_semaphore()
    for neighbour in (mate, left, right):
        pl.semaphore_signal(barrier, inc=1, device_id={"shard": neighbour}, device_id_type=MESH)
    for copy in init_copies:
        copy.wait()
    users[0] = user_in[...].T
    pltpu.async_copy(count_row.at[0], counts.at[0], init_sem.at[0]).wait()
    keep_block(0)
    pl.semaphore_wait(barrier, 3)
    count_hop().start()
    give_block(1)
    for copy in fetch(2) + fetch(3):
        copy.start()

    def run(sweep, lap, last_first):
        row = lax.rem(side + sweep, 2)
        col = lax.rem(base + row + sweep, group)
        count = counts[lax.rem(sweep, 2), 0, col]
        item = items.at[lap]
        user = users.at[sweep]
        goal_ref = target.at[row, col // 2]
        for step in range(STEPS_MAX):
            active = step < count
            bound = jnp.where(active, jnp.inf, -jnp.inf)
            keep = jnp.where(active, 1.0 - eta * lam, 1.0)
            item_now = item[...]
            user_now = user[...]
            item_half = item_now.astype(BF16)
            user_half = user_now.astype(BF16)
            approx = product(item_half, user_half, ((1,), (0,)))
            goal = goal_ref[...]
            err = jnp.where(goal < bound, approx - goal, 0.0).astype(BF16)
            item[...] = keep * item_now - eta * product(err, user_half, ((1,), (1,)))
            if last_first and step == STEPS_MAX - 1:
                last_first()
            user[...] = keep * user_now - eta * product(item_half, err, ((0,), (0,)))
        user_hop(sweep).start()

    def arrive_user(sweep):
        @pl.when(sweep > 0)
        def _():
            user_hop(sweep - 1).wait_recv()

        @pl.when(sweep > 1)
        def _():
            user_hop(sweep - 2).wait_send()

        @pl.when(sweep == 1)
        def _():
            count_hop().wait()
            pltpu.async_copy(count_row.at[1], counts.at[1], init_sem.at[0]).wait()

        @pl.when(jnp.logical_and(lax.rem(sweep, 2) == 1, sweep < group))
        def _():
            block_hop(sweep).wait_recv()

    def first_user(sweep, lap):
        arrive_user(sweep)

        @pl.when(lap > 0)
        def _():
            item_hop(lap - 1).wait_recv()

        run(sweep, lap, None)

    def second_user(sweep, lap):
        arrive_user(sweep)

        @pl.when(lap > 0)
        def _():
            item_hop(lap - 1).wait_send()

        run(sweep, lap, lambda: item_hop(lap).start())

    def lap_run(lap, _):
        second = 2 * lap + side

        @pl.when(jnp.logical_or(lap > 0, side == 1))
        def _():
            first_user(second - 1, lap)

        second_user(second, lap)

        @pl.when(2 * lap + 2 < group)
        def _():
            keep_block(2 * lap + 2)

            @pl.when(lap > 0)
            def _():
                block_hop(2 * lap - 1).wait_send()

            give_block(2 * lap + 3)

            @pl.when(2 * lap + 4 < group)
            def _():
                for copy in fetch(2 * lap + 4) + fetch(2 * lap + 5):
                    copy.start()

        return 0

    lax.fori_loop(0, laps, lap_run, 0)

    @pl.when(side == 0)
    def _():
        first_user(sweeps - 1, laps)

    @pl.when(side == 1)
    def _():
        item_hop(laps - 1).wait_recv()

    user_hop(sweeps - 1).wait_recv()
    user_out[...] = users[sweeps].T
    item_out[...] = items[laps]
    item_hop(laps - 1).wait_send()
    user_hop(sweeps - 2).wait_send()
    user_hop(sweeps - 1).wait_send()
    block_hop(group - 3).wait_send()
    block_hop(group - 1).wait_send()


def solution(mesh):
    group = mesh.shape["shard"]
    row_spec = P(("rep", "shard"), None)

    def local_run(ratings, obs_mask, step_counts, user_init, item_init):
        users_dev, rank = user_init.shape
        items_dev = item_init.shape[0]
        sweeps = EPOCHS * group
        vmem = pl.BlockSpec(memory_space=pltpu.VMEM)
        hbm = pl.BlockSpec(memory_space=pltpu.HBM)
        dma = pltpu.SemaphoreType.DMA
        return pl.pallas_call(
            functools.partial(factor_kernel, group),
            out_shape=(
                jax.ShapeDtypeStruct(user_init.shape, F32),
                jax.ShapeDtypeStruct(item_init.shape, F32),
            ),
            in_specs=[hbm] * 5,
            out_specs=(vmem, vmem),
            scratch_shapes=[
                pltpu.VMEM((sweeps // 2 + 1, items_dev, rank), F32),
                pltpu.VMEM((sweeps + 1, rank, users_dev), F32),
                pltpu.VMEM((2, group // 2, items_dev, users_dev), F32),
                pltpu.VMEM((2, items_dev, users_dev), F32),
                pltpu.VMEM((2, users_dev, items_dev), F32),
                pltpu.VMEM((2, users_dev, items_dev), jnp.int32),
                pltpu.VMEM(user_init.shape, F32),
                pltpu.VMEM((2, *step_counts.shape), jnp.int32),
                pltpu.SMEM((2, *step_counts.shape), jnp.int32),
                dma((1,)),
                dma((sweeps // 2,)),
                dma((2,)),
                dma((2,)),
                dma((2,)),
                dma((group // 2,)),
                dma((2,)),
                dma((2,)),
                dma,
                dma,
                dma((3,)),
            ],
            compiler_params=pltpu.CompilerParams(
                collective_id=0, has_side_effects=True, vmem_limit_bytes=40 * 1024 * 1024
            ),
            name="factor_ring",
        )(ratings, obs_mask, step_counts, user_init, item_init)

    return jax.shard_map(local_run, mesh=mesh, in_specs=(row_spec,) * 5, out_specs=(row_spec, row_spec), check_vma=False)
```

```python
import functools
import math

import jax
import jax.numpy as jnp
from jax import lax
from jax.experimental import pallas as pl
from jax.experimental.pallas import tpu as pltpu
from jax.sharding import PartitionSpec as P

EPOCHS = 2
STEPS_MAX = 6
MESH = pl.DeviceIdType.MESH
F32 = jnp.float32
BF16 = jnp.bfloat16


def product(a, b, contract):
    return lax.dot_general(a, b, (contract, ((), ())), preferred_element_type=F32)


def factor_kernel(group, ratings, obs_mask, step_counts, user_init, item_init, user_out, item_out,
                  items, users, target, outbox, rating_in, mask_in, user_in, count_row, counts,
                  item_send, item_recv, user_send, user_recv, block_send, block_recv,
                  rating_sem, mask_sem, count_send, count_recv, init_sem, user_first, first_send, first_recv):
    users_dev, rank = user_init.shape
    items_dev = item_init.shape[0]
    sweeps = EPOCHS * group
    laps = sweeps // 2
    eta = 0.4 * math.sqrt(rank) / (users_dev + rank)
    lam = 0.1 * items_dev / math.sqrt(rank)
    me = lax.axis_index("shard")
    side = lax.rem(me, 2)
    base = me - side
    mate = base + 1 - side
    flip = lax.rem(me // 2, 2)
    part = lax.rem(side + flip, 2)
    before = lax.rem(base + group - 2, group)
    after = lax.rem(base + 2, group)

    def fetch(sweep):
        col = lax.rem(me + sweep, group)
        cols = pl.ds(pl.multiple_of(col * items_dev, items_dev), items_dev)
        half = lax.rem(sweep, 2)
        return (
            pltpu.make_async_copy(ratings.at[:, cols], rating_in.at[half], rating_sem.at[half]),
            pltpu.make_async_copy(obs_mask.at[:, cols], mask_in.at[half], mask_sem.at[half]),
        )

    def to_mate(src, dst, send_sem, recv_sem):
        return pltpu.make_async_remote_copy(
            src_ref=src, dst_ref=dst, send_sem=send_sem, recv_sem=recv_sem,
            device_id={"shard": mate}, device_id_type=MESH)

    def item_hop(lap):
        home = jnp.where(lap == laps - 1, part, 0)
        return pltpu.make_async_remote_copy(
            src_ref=items.at[lap], dst_ref=items.at[lap + 1 + home], send_sem=item_send.at[0],
            recv_sem=item_recv.at[lap + home],
            device_id={"shard": before + jnp.where(home == 1, 1, 1 - side)}, device_id_type=MESH)

    def item_arrival(slot):
        return pltpu.make_async_remote_copy(
            src_ref=items.at[slot], dst_ref=items.at[slot], send_sem=item_send.at[0], recv_sem=item_recv.at[slot - 1],
            device_id={"shard": after + 1 - side}, device_id_type=MESH)

    def item_home():
        return to_mate(items.at[laps], items.at[laps + 1], item_send.at[0], item_recv.at[laps])

    def user_hop(sweep):
        half = lax.rem(sweep, 2)
        return to_mate(users.at[sweep], users.at[sweep + 1], user_send.at[half], user_recv.at[half])

    def block_hop(sweep):
        col = lax.rem(me + sweep, group)
        half = lax.rem(sweep // 2, 2)
        return to_mate(outbox.at[half], target.at[side, col // 2], block_send.at[half], block_recv.at[sweep // 2])

    def count_hop():
        return to_mate(count_row.at[0], count_row.at[1], count_send, count_recv)

    def merged(sweep):
        for copy in fetch(sweep):
            copy.wait()
        half = lax.rem(sweep, 2)
        return jnp.where(mask_in[half] != 0, rating_in[half], jnp.inf).T

    def keep_block(sweep):
        target[side, lax.rem(me + sweep, group) // 2] = merged(sweep)

    def give_block(sweep):
        outbox[lax.rem(sweep // 2, 2)] = merged(sweep)
        block_hop(sweep).start()

    def prepare(sweep):
        @pl.when(flip == 0)
        def _():
            keep_block(sweep)
            give_block(sweep + 1)

        @pl.when(flip == 1)
        def _():
            give_block(sweep)
            keep_block(sweep + 1)

        @pl.when(sweep + 2 < group)
        def _():
            for copy in fetch(sweep + 2) + fetch(sweep + 3):
                copy.start()

    def first_hops():
        return (
            to_mate(user_first, users.at[0], first_send.at[0], first_recv.at[0]),
            to_mate(item_init, items.at[0], first_send.at[1], first_recv.at[1]),
        )

    init_copies = (
        pltpu.make_async_copy(user_init, user_in, init_sem.at[0]),
        pltpu.make_async_copy(step_counts, count_row.at[0], init_sem.at[1]),
    )
    item_copy = pltpu.make_async_copy(item_init, items.at[0], init_sem.at[2])
    for copy in init_copies + fetch(0) + fetch(1):
        copy.start()
    pl.when(flip == 0)(item_copy.start)
    barrier = pltpu.get_barrier_semaphore()
    for neighbour in (mate, before, before + 1, after, after + 1):
        pl.semaphore_signal(barrier, inc=1, device_id={"shard": neighbour}, device_id_type=MESH)
    for copy in init_copies:
        copy.wait()
    user_first[...] = user_in[...].T
    pltpu.async_copy(count_row.at[0], counts.at[0], init_sem.at[0]).wait()
    pl.semaphore_wait(barrier, 5)
    count_hop().start()

    @pl.when(flip == 1)
    def _():
        for hop in first_hops():
            hop.start()

    @pl.when(flip == 0)
    def _():
        users[0] = user_first[...]

    prepare(0)

    def run(sweep, lap, last_first):
        row = lax.rem(part + sweep, 2)
        col = lax.rem(base + row + sweep, group)
        count = counts[lax.rem(sweep + flip, 2), 0, col]
        item = items.at[lap]
        user = users.at[sweep]
        goal_ref = target.at[row, col // 2]
        for step in range(STEPS_MAX):
            active = step < count
            bound = jnp.where(active, jnp.inf, -jnp.inf)
            keep = jnp.where(active, 1.0 - eta * lam, 1.0)
            item_now = item[...]
            user_now = user[...]
            item_half = item_now.astype(BF16)
            user_half = user_now.astype(BF16)
            approx = product(item_half, user_half, ((1,), (0,)))
            goal = goal_ref[...]
            err = jnp.where(goal < bound, approx - goal, 0.0).astype(BF16)
            item[...] = keep * item_now - eta * product(err, user_half, ((1,), (1,)))
            if last_first and step == STEPS_MAX - 1:
                last_first()
            user[...] = keep * user_now - eta * product(item_half, err, ((0,), (0,)))
        user_hop(sweep).start()

    def arrive(sweep):
        @pl.when(sweep == 1 - flip)
        def _():
            count_hop().wait()
            pltpu.async_copy(count_row.at[1], counts.at[1], init_sem.at[0]).wait()

        @pl.when(sweep > 0)
        def _():
            user_hop(sweep - 1).wait_recv()

        @pl.when(sweep > 1)
        def _():
            user_hop(sweep - 2).wait_send()

        @pl.when(jnp.logical_and(lax.rem(sweep + flip, 2) == 1, sweep < group))
        def _():
            block_hop(sweep).wait_recv()

        @pl.when(sweep == 0)
        def _():
            @pl.when(flip == 1)
            def _():
                for hop in first_hops():
                    hop.wait()

            @pl.when(flip == 0)
            def _():
                item_copy.wait()

    def first_user(sweep, lap):
        arrive(sweep)

        @pl.when(lap > 0)
        def _():
            item_arrival(lap).wait_recv()

        run(sweep, lap, None)

    def second_user(sweep, lap):
        arrive(sweep)

        @pl.when(lap > 0)
        def _():
            item_hop(lap - 1).wait_send()

        run(sweep, lap, lambda: item_hop(lap).start())

    def lap_run(lap, _):
        second = 2 * lap + part

        @pl.when(jnp.logical_or(lap > 0, part == 1))
        def _():
            first_user(second - 1, lap)

        second_user(second, lap)

        @pl.when(lap == 0)
        def _():
            prepare(2)

        @pl.when(2 * lap + 4 < group)
        def _():
            block_hop(2 * lap + 1 - flip).wait_send()
            prepare(2 * lap + 4)

        return 0

    lax.fori_loop(0, laps, lap_run, 0)
    at_home = jnp.logical_and(side == 0, flip == 0)

    @pl.when(part == 0)
    def _():
        item_hop(laps - 1).wait_send()
        first_user(sweeps - 1, laps)
        pl.when(flip == 1)(lambda: item_home().start())

    user_hop(sweeps - 1).wait_recv()
    user_out[...] = users[sweeps - flip].T

    @pl.when(jnp.logical_not(at_home))
    def _():
        item_arrival(laps + 1).wait_recv()

    item_out[...] = items[laps + jnp.where(at_home, 0, 1)]

    @pl.when(jnp.logical_not(at_home))
    def _():
        item_home().wait_send()

    user_hop(sweeps - 2).wait_send()
    user_hop(sweeps - 1).wait_send()
    block_hop(group - 3 - flip).wait_send()
    block_hop(group - 1 - flip).wait_send()


def solution(mesh):
    group = mesh.shape["shard"]
    row_spec = P(("rep", "shard"), None)

    def local_run(ratings, obs_mask, step_counts, user_init, item_init):
        users_dev, rank = user_init.shape
        items_dev = item_init.shape[0]
        sweeps = EPOCHS * group
        vmem = pl.BlockSpec(memory_space=pltpu.VMEM)
        hbm = pl.BlockSpec(memory_space=pltpu.HBM)
        dma = pltpu.SemaphoreType.DMA
        return pl.pallas_call(
            functools.partial(factor_kernel, group),
            out_shape=(
                jax.ShapeDtypeStruct(user_init.shape, F32),
                jax.ShapeDtypeStruct(item_init.shape, F32),
            ),
            in_specs=[hbm] * 5,
            out_specs=(vmem, vmem),
            scratch_shapes=[
                pltpu.VMEM((sweeps // 2 + 2, items_dev, rank), F32),
                pltpu.VMEM((sweeps + 1, rank, users_dev), F32),
                pltpu.VMEM((2, group // 2, items_dev, users_dev), F32),
                pltpu.VMEM((2, items_dev, users_dev), F32),
                pltpu.VMEM((2, users_dev, items_dev), F32),
                pltpu.VMEM((2, users_dev, items_dev), jnp.int32),
                pltpu.VMEM(user_init.shape, F32),
                pltpu.VMEM((2, *step_counts.shape), jnp.int32),
                pltpu.SMEM((2, *step_counts.shape), jnp.int32),
                dma((1,)),
                dma((sweeps // 2 + 1,)),
                dma((2,)),
                dma((2,)),
                dma((2,)),
                dma((group // 2,)),
                dma((2,)),
                dma((2,)),
                dma,
                dma,
                dma((3,)),
                pltpu.VMEM((rank, users_dev), F32),
                dma((2,)),
                dma((2,)),
            ],
            compiler_params=pltpu.CompilerParams(
                collective_id=0, has_side_effects=True, vmem_limit_bytes=40 * 1024 * 1024
            ),
            name="factor_ring",
        )(ratings, obs_mask, step_counts, user_init, item_init)

    return jax.shard_map(local_run, mesh=mesh, in_specs=(row_spec,) * 5, out_specs=(row_spec, row_spec), check_vma=False)
```

```python
import functools
import math

import jax
import jax.numpy as jnp
from jax import lax
from jax.experimental import pallas as pl
from jax.experimental.pallas import tpu as pltpu
from jax.sharding import PartitionSpec as P

EPOCHS = 2
STEPS_MAX = 6
MESH = pl.DeviceIdType.MESH
F32 = jnp.float32
BF16 = jnp.bfloat16


def product(a, b, contract):
    return lax.dot_general(a, b, (contract, ((), ())), preferred_element_type=F32)


def factor_kernel(group, ratings, obs_mask, step_counts, user_init, item_init, user_out, item_out,
                  items, users, target, outbox, rating_in, mask_in, user_in, count_row, counts,
                  item_send, item_recv, user_send, user_recv, block_send, block_recv,
                  rating_sem, mask_sem, count_send, count_recv, init_sem, user_first, first_send, first_recv):
    users_dev, rank = user_init.shape
    items_dev = item_init.shape[0]
    sweeps = EPOCHS * group
    laps = sweeps // 2
    eta = 0.4 * math.sqrt(rank) / (users_dev + rank)
    lam = 0.1 * items_dev / math.sqrt(rank)
    me = lax.axis_index("shard")
    side = lax.rem(me, 2)
    base = me - side
    mate = base + 1 - side
    flip = lax.rem(me // 2, 2)
    part = lax.rem(side + flip, 2)
    before = lax.rem(base + group - 2, group)
    after = lax.rem(base + 2, group)

    def fetch(sweep):
        col = lax.rem(me + sweep, group)
        cols = pl.ds(pl.multiple_of(col * items_dev, items_dev), items_dev)
        half = lax.rem(sweep, 2)
        return (
            pltpu.make_async_copy(ratings.at[:, cols], rating_in.at[half], rating_sem.at[half]),
            pltpu.make_async_copy(obs_mask.at[:, cols], mask_in.at[half], mask_sem.at[half]),
        )

    def to_mate(src, dst, send_sem, recv_sem):
        return pltpu.make_async_remote_copy(
            src_ref=src, dst_ref=dst, send_sem=send_sem, recv_sem=recv_sem,
            device_id={"shard": mate}, device_id_type=MESH)

    def item_hop(lap):
        home = jnp.where(lap == laps - 1, part, 0)
        return pltpu.make_async_remote_copy(
            src_ref=items.at[lap], dst_ref=items.at[lap + 1 + home], send_sem=item_send.at[0],
            recv_sem=item_recv.at[lap + home],
            device_id={"shard": before + jnp.where(home == 1, 1, 1 - side)}, device_id_type=MESH)

    def item_arrival(slot):
        return pltpu.make_async_remote_copy(
            src_ref=items.at[slot], dst_ref=items.at[slot], send_sem=item_send.at[0], recv_sem=item_recv.at[slot - 1],
            device_id={"shard": after + 1 - side}, device_id_type=MESH)

    def item_home():
        return to_mate(items.at[laps], items.at[laps + 1], item_send.at[0], item_recv.at[laps])

    def user_hop(sweep):
        half = lax.rem(sweep, 2)
        return to_mate(users.at[sweep], users.at[sweep + 1], user_send.at[half], user_recv.at[half])

    def block_hop(sweep):
        col = lax.rem(me + sweep, group)
        half = lax.rem(sweep // 2, 2)
        return to_mate(outbox.at[half], target.at[side, col // 2], block_send.at[half], block_recv.at[sweep // 2])

    def count_hop():
        return to_mate(count_row.at[0], count_row.at[1], count_send, count_recv)

    def merged(sweep):
        for copy in fetch(sweep):
            copy.wait()
        half = lax.rem(sweep, 2)
        return jnp.where(mask_in[half] != 0, rating_in[half], jnp.inf).T

    def keep_block(sweep):
        target[side, lax.rem(me + sweep, group) // 2] = merged(sweep)

    def give_block(sweep):
        outbox[lax.rem(sweep // 2, 2)] = merged(sweep)
        block_hop(sweep).start()

    def prepare(sweep):
        @pl.when(flip == 0)
        def _():
            keep_block(sweep)
            give_block(sweep + 1)

        @pl.when(flip == 1)
        def _():
            give_block(sweep)
            keep_block(sweep + 1)

        @pl.when(sweep + 2 < group)
        def _():
            for copy in fetch(sweep + 2) + fetch(sweep + 3):
                copy.start()

    def first_hops():
        return (
            to_mate(user_first, users.at[0], first_send.at[0], first_recv.at[0]),
            to_mate(item_init, items.at[0], first_send.at[1], first_recv.at[1]),
        )

    init_copies = (
        pltpu.make_async_copy(user_init, user_in, init_sem.at[0]),
        pltpu.make_async_copy(step_counts, count_row.at[0], init_sem.at[1]),
    )
    item_copy = pltpu.make_async_copy(item_init, items.at[0], init_sem.at[2])
    for copy in init_copies + fetch(0) + fetch(1):
        copy.start()
    pl.when(flip == 0)(item_copy.start)
    barrier = pltpu.get_barrier_semaphore()
    for neighbour in (mate, before, before + 1, after, after + 1):
        pl.semaphore_signal(barrier, inc=1, device_id={"shard": neighbour}, device_id_type=MESH)
    for copy in init_copies:
        copy.wait()
    user_first[...] = user_in[...].T
    pltpu.async_copy(count_row.at[0], counts.at[0], init_sem.at[0]).wait()
    pl.semaphore_wait(barrier, 5)
    count_hop().start()

    @pl.when(flip == 1)
    def _():
        for hop in first_hops():
            hop.start()

    @pl.when(flip == 0)
    def _():
        users[0] = user_first[...]

    prepare(0)

    def run(sweep, lap, last_first):
        row = lax.rem(part + sweep, 2)
        col = lax.rem(base + row + sweep, group)
        count = counts[lax.rem(sweep + flip, 2), 0, col]
        item = items.at[lap]
        user = users.at[sweep]
        goal_ref = target.at[row, col // 2]
        for step in range(STEPS_MAX):
            active = step < count
            bound = jnp.where(active, jnp.inf, -jnp.inf)
            keep = jnp.where(active, 1.0 - eta * lam, 1.0)
            item_now = item[...]
            user_now = user[...]
            item_half = item_now.astype(BF16)
            user_half = user_now.astype(BF16)
            approx = product(item_half, user_half, ((1,), (0,)))
            goal = goal_ref[...]
            err = jnp.where(goal < bound, approx - goal, 0.0).astype(BF16)
            item[...] = keep * item_now - eta * product(err, user_half, ((1,), (1,)))
            if last_first and step == STEPS_MAX - 1:
                last_first()
            user[...] = keep * user_now - eta * product(item_half, err, ((0,), (0,)))
        user_hop(sweep).start()

    def arrive(sweep):
        @pl.when(sweep == 1 - flip)
        def _():
            count_hop().wait()
            pltpu.async_copy(count_row.at[1], counts.at[1], init_sem.at[0]).wait()

        @pl.when(sweep > 0)
        def _():
            user_hop(sweep - 1).wait_recv()

        @pl.when(sweep > 1)
        def _():
            user_hop(sweep - 2).wait_send()

        @pl.when(jnp.logical_and(lax.rem(sweep + flip, 2) == 1, sweep < group))
        def _():
            block_hop(sweep).wait_recv()

        @pl.when(sweep == 0)
        def _():
            @pl.when(flip == 1)
            def _():
                for hop in first_hops():
                    hop.wait()

            @pl.when(flip == 0)
            def _():
                item_copy.wait()

    def first_user(sweep, lap):
        arrive(sweep)

        @pl.when(lap > 0)
        def _():
            item_arrival(lap).wait_recv()

        run(sweep, lap, None)

    def second_user(sweep, lap):
        arrive(sweep)

        @pl.when(lap > 0)
        def _():
            item_hop(lap - 1).wait_send()

        run(sweep, lap, lambda: item_hop(lap).start())

    def lap_run(lap, _):
        second = 2 * lap + part

        @pl.when(jnp.logical_or(lap > 0, part == 1))
        def _():
            first_user(second - 1, lap)

        second_user(second, lap)

        @pl.when(lap == 0)
        def _():
            prepare(2)

        @pl.when(2 * lap + 4 < group)
        def _():
            block_hop(2 * lap + 1 - flip).wait_send()
            prepare(2 * lap + 4)

        return 0

    lax.fori_loop(0, laps, lap_run, 0)
    at_home = jnp.logical_and(side == 0, flip == 0)

    @pl.when(part == 0)
    def _():
        item_hop(laps - 1).wait_send()
        first_user(sweeps - 1, laps)
        pl.when(flip == 1)(lambda: item_home().start())

    user_hop(sweeps - 1).wait_recv()
    user_out[...] = users[sweeps - flip].T

    @pl.when(jnp.logical_not(at_home))
    def _():
        item_arrival(laps + 1).wait_recv()

    item_out[...] = items[laps + jnp.where(at_home, 0, 1)]

    @pl.when(jnp.logical_not(at_home))
    def _():
        item_home().wait_send()

    user_hop(sweeps - 2).wait_send()
    user_hop(sweeps - 1).wait_send()
    block_hop(group - 3 - flip).wait_send()
    block_hop(group - 1 - flip).wait_send()


def solution(mesh):
    group = mesh.shape["shard"]
    row_spec = P(("rep", "shard"), None)

    def local_run(ratings, obs_mask, step_counts, user_init, item_init):
        users_dev, rank = user_init.shape
        items_dev = item_init.shape[0]
        sweeps = EPOCHS * group
        vmem = pl.BlockSpec(memory_space=pltpu.VMEM)
        hbm = pl.BlockSpec(memory_space=pltpu.HBM)
        dma = pltpu.SemaphoreType.DMA
        return pl.pallas_call(
            functools.partial(factor_kernel, group),
            out_shape=(
                jax.ShapeDtypeStruct(user_init.shape, F32),
                jax.ShapeDtypeStruct(item_init.shape, F32),
            ),
            in_specs=[hbm] * 5,
            out_specs=(vmem, vmem),
            scratch_shapes=[
                pltpu.VMEM((sweeps // 2 + 2, items_dev, rank), F32),
                pltpu.VMEM((sweeps + 1, rank, users_dev), F32),
                pltpu.VMEM((2, group // 2, items_dev, users_dev), F32),
                pltpu.VMEM((2, items_dev, users_dev), F32),
                pltpu.VMEM((2, users_dev, items_dev), F32),
                pltpu.VMEM((2, users_dev, items_dev), jnp.int32),
                pltpu.VMEM(user_init.shape, F32),
                pltpu.VMEM((2, *step_counts.shape), jnp.int32),
                pltpu.SMEM((2, *step_counts.shape), jnp.int32),
                dma((1,)),
                dma((sweeps // 2 + 1,)),
                dma((2,)),
                dma((2,)),
                dma((2,)),
                dma((group // 2,)),
                dma((2,)),
                dma((2,)),
                dma,
                dma,
                dma((3,)),
                pltpu.VMEM((rank, users_dev), F32),
                dma((2,)),
                dma((2,)),
            ],
            compiler_params=pltpu.CompilerParams(
                collective_id=0, has_side_effects=True, vmem_limit_bytes=40 * 1024 * 1024
            ),
            name="factor_ring",
        )(*(pltpu.with_memory_space_constraint(a, pltpu.HBM) for a in (ratings, obs_mask, step_counts, user_init, item_init)))

    return jax.shard_map(local_run, mesh=mesh, in_specs=(row_spec,) * 5, out_specs=(row_spec, row_spec), check_vma=False)
```

```python
import functools
import math

import jax
import jax.numpy as jnp
from jax import lax
from jax.experimental import pallas as pl
from jax.experimental.pallas import tpu as pltpu
from jax.sharding import PartitionSpec as P

EPOCHS = 2
STEPS_MAX = 6
PIECES = 2
MESH = pl.DeviceIdType.MESH
F32 = jnp.float32
BF16 = jnp.bfloat16


def product(a, b, contract):
    return lax.dot_general(a, b, (contract, ((), ())), preferred_element_type=F32)


def factor_kernel(group, ratings, obs_mask, step_counts, user_init, item_init, user_out, item_out,
                  items, users, target, outbox, rating_in, mask_in, user_in, count_row, counts,
                  item_send, item_recv, user_send, user_recv, block_send, block_recv,
                  rating_sem, mask_sem, count_send, count_recv, init_sem, user_first, first_send, first_recv):
    users_dev, rank = user_init.shape
    items_dev = item_init.shape[0]
    sweeps = EPOCHS * group
    laps = sweeps // 2
    eta = 0.4 * math.sqrt(rank) / (users_dev + rank)
    lam = 0.1 * items_dev / math.sqrt(rank)
    me = lax.axis_index("shard")
    side = lax.rem(me, 2)
    base = me - side
    mate = base + 1 - side
    flip = lax.rem(me // 2, 2)
    part = lax.rem(side + flip, 2)
    before = lax.rem(base + group - 2, group)
    after = lax.rem(base + 2, group)

    def fetch(sweep):
        col = lax.rem(me + sweep, group)
        cols = pl.ds(pl.multiple_of(col * items_dev, items_dev), items_dev)
        half = lax.rem(sweep, 2)
        return (
            pltpu.make_async_copy(ratings.at[:, cols], rating_in.at[half], rating_sem.at[half]),
            pltpu.make_async_copy(obs_mask.at[:, cols], mask_in.at[half], mask_sem.at[half]),
        )

    def to_mate(src, dst, send_sem, recv_sem):
        return pltpu.make_async_remote_copy(
            src_ref=src, dst_ref=dst, send_sem=send_sem, recv_sem=recv_sem,
            device_id={"shard": mate}, device_id_type=MESH)

    def rows(piece):
        return pl.ds(piece * (items_dev // PIECES), items_dev // PIECES)

    def item_hop(lap, piece):
        home = jnp.where(lap == laps - 1, part, 0)
        return pltpu.make_async_remote_copy(
            src_ref=items.at[lap, rows(piece)], dst_ref=items.at[lap + 1 + home, rows(piece)],
            send_sem=item_send.at[piece], recv_sem=item_recv.at[lap + 1 + home, piece],
            device_id={"shard": before + jnp.where(home == 1, 1, 1 - side)}, device_id_type=MESH)

    def item_arrival(slot, piece):
        return pltpu.make_async_remote_copy(
            src_ref=items.at[slot, rows(piece)], dst_ref=items.at[slot, rows(piece)],
            send_sem=item_send.at[piece], recv_sem=item_recv.at[slot, piece],
            device_id={"shard": after + 1 - side}, device_id_type=MESH)

    def item_home(piece):
        return to_mate(items.at[laps, rows(piece)], items.at[laps + 1, rows(piece)],
                       item_send.at[piece], item_recv.at[laps + 1, piece])

    def user_hop(sweep):
        half = lax.rem(sweep, 2)
        return to_mate(users.at[sweep], users.at[sweep + 1], user_send.at[half], user_recv.at[half])

    def block_hop(sweep):
        col = lax.rem(me + sweep, group)
        half = lax.rem(sweep // 2, 2)
        return to_mate(outbox.at[half], target.at[side, col // 2], block_send.at[half], block_recv.at[sweep // 2])

    def count_hop():
        return to_mate(count_row.at[0], count_row.at[1], count_send, count_recv)

    def merged(sweep):
        for copy in fetch(sweep):
            copy.wait()
        half = lax.rem(sweep, 2)
        return jnp.where(mask_in[half] != 0, rating_in[half], jnp.inf).T

    def keep_block(sweep):
        target[side, lax.rem(me + sweep, group) // 2] = merged(sweep)

    def give_block(sweep):
        outbox[lax.rem(sweep // 2, 2)] = merged(sweep)
        block_hop(sweep).start()

    def prepare(sweep):
        @pl.when(flip == 0)
        def _():
            keep_block(sweep)
            give_block(sweep + 1)

        @pl.when(flip == 1)
        def _():
            give_block(sweep)
            keep_block(sweep + 1)

        @pl.when(sweep + 2 < group)
        def _():
            for copy in fetch(sweep + 2) + fetch(sweep + 3):
                copy.start()

    user_first_hop = to_mate(user_first, users.at[0], first_send.at[0], first_recv.at[0])
    item_first_hops = [
        to_mate(item_init.at[rows(piece)], items.at[0, rows(piece)], item_send.at[piece], item_recv.at[0, piece])
        for piece in range(PIECES)
    ]
    item_copies = [
        pltpu.make_async_copy(item_init.at[rows(piece)], items.at[0, rows(piece)], item_recv.at[0, piece])
        for piece in range(PIECES)
    ]

    init_copies = (
        pltpu.make_async_copy(user_init, user_in, init_sem.at[0]),
        pltpu.make_async_copy(step_counts, count_row.at[0], init_sem.at[1]),
    )
    for copy in init_copies + fetch(0) + fetch(1):
        copy.start()

    @pl.when(flip == 0)
    def _():
        for copy in item_copies:
            copy.start()

    barrier = pltpu.get_barrier_semaphore()
    for neighbour in (mate, before, before + 1, after, after + 1):
        pl.semaphore_signal(barrier, inc=1, device_id={"shard": neighbour}, device_id_type=MESH)
    for copy in init_copies:
        copy.wait()
    user_first[...] = user_in[...].T
    pltpu.async_copy(count_row.at[0], counts.at[0], init_sem.at[0]).wait()
    pl.semaphore_wait(barrier, 5)
    count_hop().start()

    @pl.when(flip == 1)
    def _():
        for hop in (user_first_hop, *item_first_hops):
            hop.start()

    @pl.when(flip == 0)
    def _():
        users[0] = user_first[...]

    prepare(0)

    def run(sweep, lap, arriving, leaving):
        row = lax.rem(part + sweep, 2)
        col = lax.rem(base + row + sweep, group)
        count = counts[lax.rem(sweep + flip, 2), 0, col]
        item = items.at[lap]
        user = users.at[sweep]
        goal_ref = target.at[row, col // 2]
        for step in range(STEPS_MAX):
            active = step < count
            bound = jnp.where(active, jnp.inf, -jnp.inf)
            keep = jnp.where(active, 1.0 - eta * lam, 1.0)
            receiving = arriving is not None and step == 0
            sending = leaving is not None and step == STEPS_MAX - 1
            pieces = PIECES if receiving or sending else 1
            size = items_dev // pieces
            user_now = user[...]
            user_half = user_now.astype(BF16)
            halves, errs = [], []
            for piece in range(pieces):
                here = pl.ds(piece * size, size)
                if receiving:
                    arriving(piece)
                item_now = item[here]
                item_half = item_now.astype(BF16)
                approx = product(item_half, user_half, ((1,), (0,)))
                goal = goal_ref[here]
                err = jnp.where(goal < bound, approx - goal, 0.0).astype(BF16)
                item[here] = keep * item_now - eta * product(err, user_half, ((1,), (1,)))
                if sending:
                    leaving(piece)
                halves.append(item_half)
                errs.append(err)
            item_half = jnp.concatenate(halves, 0) if pieces > 1 else halves[0]
            err = jnp.concatenate(errs, 0) if pieces > 1 else errs[0]
            user[...] = keep * user_now - eta * product(item_half, err, ((0,), (0,)))
        user_hop(sweep).start()

    def arrive(sweep):
        @pl.when(sweep == 1 - flip)
        def _():
            count_hop().wait()
            pltpu.async_copy(count_row.at[1], counts.at[1], init_sem.at[0]).wait()

        @pl.when(sweep > 0)
        def _():
            user_hop(sweep - 1).wait_recv()

        @pl.when(sweep > 1)
        def _():
            user_hop(sweep - 2).wait_send()

        @pl.when(jnp.logical_and(lax.rem(sweep + flip, 2) == 1, sweep < group))
        def _():
            block_hop(sweep).wait_recv()

        @pl.when(sweep == 0)
        def _():
            @pl.when(flip == 1)
            def _():
                user_first_hop.wait()
                for hop in item_first_hops:
                    hop.wait_send()

    def first_user(sweep, lap):
        arrive(sweep)
        run(sweep, lap, lambda piece: item_arrival(lap, piece).wait_recv(), None)

    def second_user(sweep, lap):
        arrive(sweep)

        @pl.when(jnp.logical_and(lap == 0, part == 0))
        def _():
            for piece in range(PIECES):
                item_arrival(0, piece).wait_recv()

        @pl.when(lap > 0)
        def _():
            for piece in range(PIECES):
                item_hop(lap - 1, piece).wait_send()

        run(sweep, lap, None, lambda piece: item_hop(lap, piece).start())

    def lap_run(lap, _):
        second = 2 * lap + part

        @pl.when(jnp.logical_or(lap > 0, part == 1))
        def _():
            first_user(second - 1, lap)

        second_user(second, lap)

        @pl.when(lap == 0)
        def _():
            prepare(2)

        @pl.when(2 * lap + 4 < group)
        def _():
            block_hop(2 * lap + 1 - flip).wait_send()
            prepare(2 * lap + 4)

        return 0

    lax.fori_loop(0, laps, lap_run, 0)
    at_home = jnp.logical_and(side == 0, flip == 0)

    @pl.when(part == 0)
    def _():
        for piece in range(PIECES):
            item_hop(laps - 1, piece).wait_send()
        first_user(sweeps - 1, laps)

        @pl.when(flip == 1)
        def _():
            for piece in range(PIECES):
                item_home(piece).start()

    user_hop(sweeps - 1).wait_recv()
    user_out[...] = users[sweeps - flip].T

    @pl.when(jnp.logical_not(at_home))
    def _():
        for piece in range(PIECES):
            item_arrival(laps + 1, piece).wait_recv()

    item_out[...] = items[laps + jnp.where(at_home, 0, 1)]

    @pl.when(jnp.logical_not(at_home))
    def _():
        for piece in range(PIECES):
            item_home(piece).wait_send()

    user_hop(sweeps - 2).wait_send()
    user_hop(sweeps - 1).wait_send()
    block_hop(group - 3 - flip).wait_send()
    block_hop(group - 1 - flip).wait_send()


def solution(mesh):
    group = mesh.shape["shard"]
    row_spec = P(("rep", "shard"), None)

    def local_run(ratings, obs_mask, step_counts, user_init, item_init):
        users_dev, rank = user_init.shape
        items_dev = item_init.shape[0]
        sweeps = EPOCHS * group
        vmem = pl.BlockSpec(memory_space=pltpu.VMEM)
        hbm = pl.BlockSpec(memory_space=pltpu.HBM)
        dma = pltpu.SemaphoreType.DMA
        return pl.pallas_call(
            functools.partial(factor_kernel, group),
            out_shape=(
                jax.ShapeDtypeStruct(user_init.shape, F32),
                jax.ShapeDtypeStruct(item_init.shape, F32),
            ),
            in_specs=[hbm] * 5,
            out_specs=(vmem, vmem),
            scratch_shapes=[
                pltpu.VMEM((sweeps // 2 + 2, items_dev, rank), F32),
                pltpu.VMEM((sweeps + 1, rank, users_dev), F32),
                pltpu.VMEM((2, group // 2, items_dev, users_dev), F32),
                pltpu.VMEM((2, items_dev, users_dev), F32),
                pltpu.VMEM((2, users_dev, items_dev), F32),
                pltpu.VMEM((2, users_dev, items_dev), jnp.int32),
                pltpu.VMEM(user_init.shape, F32),
                pltpu.VMEM((2, *step_counts.shape), jnp.int32),
                pltpu.SMEM((2, *step_counts.shape), jnp.int32),
                dma((PIECES,)),
                dma((sweeps // 2 + 2, PIECES)),
                dma((2,)),
                dma((2,)),
                dma((2,)),
                dma((group // 2,)),
                dma((2,)),
                dma((2,)),
                dma,
                dma,
                dma((3,)),
                pltpu.VMEM((rank, users_dev), F32),
                dma((1,)),
                dma((1,)),
            ],
            compiler_params=pltpu.CompilerParams(
                collective_id=0, has_side_effects=True, vmem_limit_bytes=40 * 1024 * 1024
            ),
            name="factor_ring",
        )(*(pltpu.with_memory_space_constraint(a, pltpu.HBM) for a in (ratings, obs_mask, step_counts, user_init, item_init)))

    return jax.shard_map(local_run, mesh=mesh, in_specs=(row_spec,) * 5, out_specs=(row_spec, row_spec), check_vma=False)
```

```python
import functools
import math

import jax
import jax.numpy as jnp
from jax import lax
from jax.experimental import pallas as pl
from jax.experimental.pallas import tpu as pltpu
from jax.sharding import PartitionSpec as P

EPOCHS = 2
STEPS_MAX = 6
PIECES = 2
MESH = pl.DeviceIdType.MESH
F32 = jnp.float32
BF16 = jnp.bfloat16


def product(a, b, contract):
    return lax.dot_general(a, b, (contract, ((), ())), preferred_element_type=F32)


def factor_kernel(group, ratings, obs_mask, step_counts, user_init, item_init, user_out, item_out,
                  items, users, target, outbox, rating_in, mask_in, user_in, count_row, counts,
                  item_send, item_recv, user_send, user_recv, block_send, block_recv,
                  rating_sem, mask_sem, count_send, count_recv, init_sem, user_first, first_send, first_recv):
    users_dev, rank = user_init.shape
    items_dev = item_init.shape[0]
    sweeps = EPOCHS * group
    laps = sweeps // 2
    eta = 0.4 * math.sqrt(rank) / (users_dev + rank)
    lam = 0.1 * items_dev / math.sqrt(rank)
    me = lax.axis_index("shard")
    side = lax.rem(me, 2)
    base = me - side
    mate = base + 1 - side
    flip = lax.rem(me // 2, 2)
    part = lax.rem(side + flip, 2)
    before = lax.rem(base + group - 2, group)
    after = lax.rem(base + 2, group)

    def fetch(sweep):
        col = lax.rem(me + sweep, group)
        cols = pl.ds(pl.multiple_of(col * items_dev, items_dev), items_dev)
        half = lax.rem(sweep, 2)
        return (
            pltpu.make_async_copy(ratings.at[:, cols], rating_in.at[half], rating_sem.at[half]),
            pltpu.make_async_copy(obs_mask.at[:, cols], mask_in.at[half], mask_sem.at[half]),
        )

    def to_mate(src, dst, send_sem, recv_sem):
        return pltpu.make_async_remote_copy(
            src_ref=src, dst_ref=dst, send_sem=send_sem, recv_sem=recv_sem,
            device_id={"shard": mate}, device_id_type=MESH)

    def rows(piece):
        return pl.ds(piece * (items_dev // PIECES), items_dev // PIECES)

    def item_hop(lap, piece):
        home = jnp.where(lap == laps - 1, part, 0)
        return pltpu.make_async_remote_copy(
            src_ref=items.at[lap, rows(piece)], dst_ref=items.at[lap + 1 + home, rows(piece)],
            send_sem=item_send.at[piece], recv_sem=item_recv.at[lap + 1 + home, piece],
            device_id={"shard": before + jnp.where(home == 1, 1, 1 - side)}, device_id_type=MESH)

    def item_arrival(slot, piece):
        return pltpu.make_async_remote_copy(
            src_ref=items.at[slot, rows(piece)], dst_ref=items.at[slot, rows(piece)],
            send_sem=item_send.at[piece], recv_sem=item_recv.at[slot, piece],
            device_id={"shard": after + 1 - side}, device_id_type=MESH)

    def item_home(piece):
        return to_mate(items.at[laps, rows(piece)], items.at[laps + 1, rows(piece)],
                       item_send.at[piece], item_recv.at[laps + 1, piece])

    def user_hop(sweep):
        half = lax.rem(sweep, 2)
        return to_mate(users.at[sweep], users.at[sweep + 1], user_send.at[half], user_recv.at[half])

    def block_hop(sweep):
        col = lax.rem(me + sweep, group)
        half = lax.rem(sweep // 2, 2)
        return to_mate(outbox.at[half], target.at[side, col // 2], block_send.at[half], block_recv.at[sweep // 2])

    def count_hop():
        return to_mate(count_row.at[0], count_row.at[1], count_send, count_recv)

    def merged(sweep):
        for copy in fetch(sweep):
            copy.wait()
        half = lax.rem(sweep, 2)
        return jnp.where(mask_in[half] != 0, rating_in[half], jnp.inf).T

    def keep_block(sweep):
        target[side, lax.rem(me + sweep, group) // 2] = merged(sweep)

    def give_block(sweep):
        outbox[lax.rem(sweep // 2, 2)] = merged(sweep)
        block_hop(sweep).start()

    def prepare(sweep):
        @pl.when(flip == 0)
        def _():
            keep_block(sweep)
            give_block(sweep + 1)

        @pl.when(flip == 1)
        def _():
            give_block(sweep)
            keep_block(sweep + 1)

        @pl.when(sweep + 2 < group)
        def _():
            for copy in fetch(sweep + 2) + fetch(sweep + 3):
                copy.start()

    user_first_hop = to_mate(user_first, users.at[0], first_send.at[0], first_recv.at[0])
    item_first_hops = [
        to_mate(item_init.at[rows(piece)], items.at[0, rows(piece)], item_send.at[piece], item_recv.at[0, piece])
        for piece in range(PIECES)
    ]
    item_copies = [
        pltpu.make_async_copy(item_init.at[rows(piece)], items.at[0, rows(piece)], item_recv.at[0, piece])
        for piece in range(PIECES)
    ]

    init_copies = (
        pltpu.make_async_copy(user_init, user_in, init_sem.at[0]),
        pltpu.make_async_copy(step_counts, count_row.at[0], init_sem.at[1]),
    )
    for copy in init_copies + fetch(0) + fetch(1):
        copy.start()

    @pl.when(flip == 0)
    def _():
        for copy in item_copies:
            copy.start()

    barrier = pltpu.get_barrier_semaphore()
    for neighbour in (mate, before, before + 1, after, after + 1):
        pl.semaphore_signal(barrier, inc=1, device_id={"shard": neighbour}, device_id_type=MESH)
    for copy in init_copies:
        copy.wait()
    user_first[...] = user_in[...].T
    pltpu.async_copy(count_row.at[0], counts.at[0], init_sem.at[0]).wait()
    pl.semaphore_wait(barrier, 5)
    count_hop().start()

    @pl.when(flip == 1)
    def _():
        for hop in (user_first_hop, *item_first_hops):
            hop.start()

    @pl.when(flip == 0)
    def _():
        users[0] = user_first[...]

    prepare(0)

    def run(sweep, lap, arriving, leaving):
        row = lax.rem(part + sweep, 2)
        col = lax.rem(base + row + sweep, group)
        count = counts[lax.rem(sweep + flip, 2), 0, col]
        item = items.at[lap]
        user = users.at[sweep]
        goal_ref = target.at[row, col // 2]
        for step in range(STEPS_MAX):
            active = step < count
            bound = jnp.where(active, jnp.inf, -jnp.inf)
            keep = jnp.where(active, 1.0 - eta * lam, 1.0)
            receiving = arriving is not None and step == 0
            sending = leaving is not None and step == STEPS_MAX - 1
            size = items_dev // PIECES
            user_now = user[...]
            user_half = user_now.astype(BF16)
            halves, errs, later = [], [], []
            for piece in range(PIECES):
                here = pl.ds(piece * size, size)
                if receiving:
                    arriving(piece)
                item_now = item[here]
                item_half = item_now.astype(BF16)
                approx = product(item_half, user_half, ((1,), (0,)))
                goal = goal_ref[here]
                err = jnp.where(goal < bound, approx - goal, 0.0).astype(BF16)
                if sending or receiving:
                    item[here] = keep * item_now - eta * product(err, user_half, ((1,), (1,)))
                else:
                    later.append((here, item_now))
                if sending:
                    leaving(piece)
                halves.append(item_half)
                errs.append(err)
            grad_user = product(jnp.concatenate(halves, 0), jnp.concatenate(errs, 0), ((0,), (0,)))
            user[...] = keep * user_now - eta * grad_user
            for (here, item_now), err in zip(later, errs):
                item[here] = keep * item_now - eta * product(err, user_half, ((1,), (1,)))
        user_hop(sweep).start()

    def arrive(sweep):
        @pl.when(sweep == 1 - flip)
        def _():
            count_hop().wait()
            pltpu.async_copy(count_row.at[1], counts.at[1], init_sem.at[0]).wait()

        @pl.when(sweep > 0)
        def _():
            user_hop(sweep - 1).wait_recv()

        @pl.when(sweep > 1)
        def _():
            user_hop(sweep - 2).wait_send()

        @pl.when(jnp.logical_and(lax.rem(sweep + flip, 2) == 1, sweep < group))
        def _():
            block_hop(sweep).wait_recv()

        @pl.when(sweep == 0)
        def _():
            @pl.when(flip == 1)
            def _():
                user_first_hop.wait()
                for hop in item_first_hops:
                    hop.wait_send()

    def first_user(sweep, lap):
        arrive(sweep)
        run(sweep, lap, lambda piece: item_arrival(lap, piece).wait_recv(), None)

    def second_user(sweep, lap):
        arrive(sweep)

        @pl.when(jnp.logical_and(lap == 0, part == 0))
        def _():
            for piece in range(PIECES):
                item_arrival(0, piece).wait_recv()

        @pl.when(lap > 0)
        def _():
            for piece in range(PIECES):
                item_hop(lap - 1, piece).wait_send()

        run(sweep, lap, None, lambda piece: item_hop(lap, piece).start())

    def lap_run(lap, _):
        second = 2 * lap + part

        @pl.when(jnp.logical_or(lap > 0, part == 1))
        def _():
            first_user(second - 1, lap)

        second_user(second, lap)

        @pl.when(lap == 0)
        def _():
            prepare(2)

        @pl.when(2 * lap + 4 < group)
        def _():
            block_hop(2 * lap + 1 - flip).wait_send()
            prepare(2 * lap + 4)

        return 0

    lax.fori_loop(0, laps, lap_run, 0)
    at_home = jnp.logical_and(side == 0, flip == 0)

    @pl.when(part == 0)
    def _():
        for piece in range(PIECES):
            item_hop(laps - 1, piece).wait_send()
        first_user(sweeps - 1, laps)

        @pl.when(flip == 1)
        def _():
            for piece in range(PIECES):
                item_home(piece).start()

    user_hop(sweeps - 1).wait_recv()
    user_out[...] = users[sweeps - flip].T

    @pl.when(jnp.logical_not(at_home))
    def _():
        for piece in range(PIECES):
            item_arrival(laps + 1, piece).wait_recv()

    item_out[...] = items[laps + jnp.where(at_home, 0, 1)]

    @pl.when(jnp.logical_not(at_home))
    def _():
        for piece in range(PIECES):
            item_home(piece).wait_send()

    user_hop(sweeps - 2).wait_send()
    user_hop(sweeps - 1).wait_send()
    block_hop(group - 3 - flip).wait_send()
    block_hop(group - 1 - flip).wait_send()


def solution(mesh):
    group = mesh.shape["shard"]
    row_spec = P(("rep", "shard"), None)

    def local_run(ratings, obs_mask, step_counts, user_init, item_init):
        users_dev, rank = user_init.shape
        items_dev = item_init.shape[0]
        sweeps = EPOCHS * group
        vmem = pl.BlockSpec(memory_space=pltpu.VMEM)
        hbm = pl.BlockSpec(memory_space=pltpu.HBM)
        dma = pltpu.SemaphoreType.DMA
        return pl.pallas_call(
            functools.partial(factor_kernel, group),
            out_shape=(
                jax.ShapeDtypeStruct(user_init.shape, F32),
                jax.ShapeDtypeStruct(item_init.shape, F32),
            ),
            in_specs=[hbm] * 5,
            out_specs=(vmem, vmem),
            scratch_shapes=[
                pltpu.VMEM((sweeps // 2 + 2, items_dev, rank), F32),
                pltpu.VMEM((sweeps + 1, rank, users_dev), F32),
                pltpu.VMEM((2, group // 2, items_dev, users_dev), F32),
                pltpu.VMEM((2, items_dev, users_dev), F32),
                pltpu.VMEM((2, users_dev, items_dev), F32),
                pltpu.VMEM((2, users_dev, items_dev), jnp.int32),
                pltpu.VMEM(user_init.shape, F32),
                pltpu.VMEM((2, *step_counts.shape), jnp.int32),
                pltpu.SMEM((2, *step_counts.shape), jnp.int32),
                dma((PIECES,)),
                dma((sweeps // 2 + 2, PIECES)),
                dma((2,)),
                dma((2,)),
                dma((2,)),
                dma((group // 2,)),
                dma((2,)),
                dma((2,)),
                dma,
                dma,
                dma((3,)),
                pltpu.VMEM((rank, users_dev), F32),
                dma((1,)),
                dma((1,)),
            ],
            compiler_params=pltpu.CompilerParams(
                collective_id=0, has_side_effects=True, vmem_limit_bytes=40 * 1024 * 1024
            ),
            name="factor_ring",
        )(*(pltpu.with_memory_space_constraint(a, pltpu.HBM) for a in (ratings, obs_mask, step_counts, user_init, item_init)))

    return jax.shard_map(local_run, mesh=mesh, in_specs=(row_spec,) * 5, out_specs=(row_spec, row_spec), check_vma=False)
```
